256 devices in a mesh: grp: 4 (over x), row: 64 (over y, z, core).
Axes of the slice: x: 4, y: 4, z: 8, core: 2. Of those that a mesh axis runs over, the one named last changes fastest.
Arguments:
- krylov_basis: bfloat16 [300, 4096, 512], P(None, 'row', 'grp'), may hold values from -30 to 30
- krylov_image: bfloat16 [300, 4096, 512], P(None, 'row', 'grp'), may hold values from -30 to 30
- tridiag_vectors: bfloat16 [300, 32], P(None, 'grp'), may hold values from -0.375 to 0.375
- ritz_values: bfloat16 [32], P('grp'), may hold values from -3 to 3
Outputs:
- ritz_vectors: float32 [32, 4096, 512], P('grp', 'row')
- ritz_residuals: float32 [32, 4096, 512], P('grp', 'row')
- residual_norms: float32 [32], P('grp')
The draws below stay inside these ranges and needn't reach their ends.
All inputs are finite; a program needn't handle non-finite values.
Results may differ from the reference program's by a relative error of at most 0.0003.
Values may be sent and summed in bfloat16 or wider, within the bound.
No kernel may reach another device: no remote copies, remote signals or barrier semaphores. Data moves between devices by JAX's collectives and lax.ppermute only.
A program may use at most 64 MiB of HBM per device.

```python
import jax
import jax.numpy as jnp
from jax import lax

KRYLOV = 300
WANTED = 32
OUTER_DEV = 64
INNER_DEV = 128
OUTER = 4096
INNER = 512
ROWS = 2097152


def block_field(key):
    key_noise, key_scale, key_coef, key_common = jax.random.split(key, 4)
    blocks_outer = OUTER // OUTER_DEV
    blocks_inner = INNER // INNER_DEV
    noise_field = jax.random.normal(key_noise, (KRYLOV, OUTER, INNER), jnp.float32)
    levels = jax.random.uniform(key_scale, (blocks_outer, blocks_inner), jnp.float32, -0.7, 0.7)
    scales = jnp.exp(levels)
    scales = jnp.repeat(jnp.repeat(scales, OUTER_DEV, axis=0), INNER_DEV, axis=1)
    values_field = noise_field * scales[None, :, :]
    return jnp.clip(values_field, -30.0, 30.0).astype(jnp.bfloat16)


def draw_krylov_basis(key, part):
    return block_field(jax.random.fold_in(key, 11))


def draw_krylov_image(key, part):
    return block_field(jax.random.fold_in(key, 23))


def shard_levels(key, extent, pieces, least, high):
    factor_of, own = 1.0, jax.random.fold_in(key, 6)
    for dim, blocks in pieces:
        steps = jnp.exp(jax.random.uniform(jax.random.fold_in(own, dim), (blocks,), jnp.float32, least / len(pieces), high / len(pieces)))
        factor_of = factor_of * jnp.repeat(steps, extent[dim] // blocks).reshape([-1 if axis == dim else 1 for axis in range(len(extent))])
    return factor_of


def noise(rng, shape, width, bound, cuts=(), dtype=jnp.bfloat16):
    drawn = jax.random.normal(rng, shape, jnp.float32) * width
    if len(cuts) > 0:
        drawn = shard_levels(rng, shape, cuts, -0.22, 0.18) * drawn
    return jnp.clip(drawn, min=-bound, max=bound).astype(dtype)


def setup_inputs(seed: int = 0) -> dict:
    key_of = jax.random.split(jax.random.key(seed), 5)
    return {
        "krylov_basis": draw_krylov_basis(jax.random.fold_in(key_of[4], 71), 0),
        "krylov_image": draw_krylov_image(jax.random.fold_in(key_of[4], 71), 0),
        "tridiag_vectors": noise(key_of[2], (KRYLOV, WANTED), KRYLOV ** -0.5, 0.375, ((1, 4),)),
        "ritz_values": jnp.clip(jax.random.uniform(key_of[3], (WANTED,), jnp.float32, -3.0, 3.0) * shard_levels(key_of[3], (WANTED,), ((0, 4),), -0.4, 0.0), -3.0, 3.0).astype(jnp.bfloat16),
    }


def reference(krylov_basis, krylov_image, tridiag_vectors, ritz_values):
    flat_basis = krylov_basis.reshape(KRYLOV, OUTER * INNER)
    flat_image = krylov_image.reshape(KRYLOV, OUTER * INNER)
    coef_rows = tridiag_vectors.T
    ritz_cols = jnp.dot(coef_rows, flat_basis, preferred_element_type=jnp.float32)
    applied = jnp.dot(coef_rows, flat_image, preferred_element_type=jnp.float32)
    shift_values = ritz_values.astype(jnp.float32)
    resid_cols = applied - shift_values[:, None] * ritz_cols
    ritz_squares = lax.optimization_barrier(jnp.sum(ritz_cols * ritz_cols, axis=1)) + 1.0
    resid_squares = lax.optimization_barrier(jnp.sum(resid_cols * resid_cols, axis=1))
    factor = jnp.sqrt(ROWS / ritz_squares)
    ritz_vectors = (ritz_cols * factor[:, None]).reshape(WANTED, OUTER, INNER)
    ritz_residuals = (resid_cols * factor[:, None]).reshape(WANTED, OUTER, INNER)
    residual_norms = jnp.sqrt(resid_squares / ritz_squares)
    return (ritz_vectors, ritz_residuals, residual_norms)
```

```python
import functools

import jax
import jax.numpy as jnp
from jax import lax
from jax.experimental import pallas as pl
from jax.experimental.pallas import tpu as pltpu
from jax.sharding import PartitionSpec as P

LANES = 128
SHIFT_AT = 384


def pack_kernel(coef_ref, value_ref, out_ref):
    cols, krylov = coef_ref.shape
    out_ref[...] = jnp.zeros_like(out_ref)
    out_ref[:, :krylov] = coef_ref[...]
    row = lax.broadcasted_iota(jnp.int32, (cols, cols), 0)
    lane = lax.broadcasted_iota(jnp.int32, (cols, cols), 1)
    values = jnp.broadcast_to(value_ref[...].astype(jnp.float32), (cols, cols))
    column = jnp.sum(jnp.where(row == lane, values, 0.0), axis=1, keepdims=True)
    out_ref[:, SHIFT_AT:] = jnp.broadcast_to(column, (cols, LANES)).astype(jnp.bfloat16)


def power_of_two(exponent, sign):
    out = jnp.ones(exponent.shape, jnp.float32)
    whole = exponent.astype(jnp.int32)
    for bit in range(7):
        out = out * jnp.where((whole & (1 << bit)) != 0, 2.0 ** (sign * (1 << bit)), 1.0)
    return out


def project_kernel(*refs, groups, per_step):
    coef_refs, (basis_ref, image_ref) = refs[:groups], refs[groups : groups + 2]
    own_ref = refs[groups + 2]
    chunk_refs = refs[groups + 3 : 2 * groups + 2]
    sum_refs = refs[2 * groups + 2 : 3 * groups + 2]
    held, squares, peaks = refs[3 * groups + 2 :]
    krylov = basis_ref.shape[0]
    cols = coef_refs[0].shape[0]
    wanted = groups * cols
    step = pl.program_id(0)

    @pl.when(step == 0)
    def _():
        squares[...] = jnp.zeros_like(squares)
        peaks[...] = jnp.zeros_like(peaks)

    coefs = jnp.concatenate([ref[:, :krylov].astype(jnp.float32) for ref in coef_refs])
    coefs = coefs.astype(jnp.bfloat16)
    shift = jnp.concatenate([ref[:, SHIFT_AT:].astype(jnp.float32) for ref in coef_refs])
    shift = jnp.concatenate([shift, shift], axis=1)
    basis = jnp.swapaxes(basis_ref[...], 0, 1)
    image = jnp.swapaxes(image_ref[...], 0, 1)
    for pair in range(0, per_step, 2):
        fields = []
        for field in (basis, image):
            both = jnp.concatenate([field[pair], field[pair + 1]], axis=1)
            fields.append(jnp.dot(coefs, both, preferred_element_type=jnp.float32))
        ritz, resid = fields[0], fields[1] - shift * fields[0]
        for at, value in ((0, ritz), (wanted, resid)):
            squares[at : at + wanted] += value * value
            peaks[at : at + wanted] = jnp.maximum(peaks[at : at + wanted], jnp.abs(value))
            for half in range(2):
                held[step * per_step + pair + half, at : at + wanted] = value[:, half * LANES : (half + 1) * LANES]

    @pl.when(step == pl.num_programs(0) - 1)
    def _():
        sums = jnp.sum(squares[...], axis=1, keepdims=True)
        row = lax.broadcasted_iota(jnp.int32, (cols, LANES), 0)
        lane = lax.broadcasted_iota(jnp.int32, (cols, LANES), 1)
        for s in range(groups):
            line = jnp.where(lane == row, sums[s * cols : (s + 1) * cols], 0.0)
            at = wanted + s * cols
            line = line + jnp.where(lane == row + cols, sums[at : at + cols], 0.0)
            sum_refs[s][...] = jnp.sum(line, axis=0, keepdims=True)
        peak = jnp.max(peaks[...], axis=1, keepdims=True)
        exponent = jnp.clip(jnp.floor(14.0 - jnp.log(peak) * 1.4426950408889634), 0.0, 100.0)
        exponent = jnp.broadcast_to(exponent, (2 * wanted, LANES))
        scale = power_of_two(exponent, 1)
        outer = held.shape[0]
        for s in range(groups):
            for which in range(2):
                at = which * wanted + s * cols
                block = jnp.swapaxes(held[:, at : at + cols, :], 0, 1)
                if s == 0:
                    own_ref[which * cols : (which + 1) * cols] = block
                else:
                    block = block * scale[at : at + cols][:, None, :]
                    ref = chunk_refs[s - 1]
                    ref[pl.ds(which * cols * outer, cols * outer), :] = block.reshape(cols * outer, LANES)
                    ref[pl.ds(2 * cols * outer + which * cols, cols), :] = exponent[at : at + cols]


def finish_kernel(*refs, groups, rows_total):
    own_ref, chunk_refs, total_ref = refs[0], refs[1:groups], refs[groups]
    outs, norm_ref = refs[groups + 1 : groups + 3], refs[groups + 3]
    double, outer, _ = own_ref.shape
    cols = double // 2
    total = jnp.sum(total_ref[...], axis=0, keepdims=True)
    row = lax.broadcasted_iota(jnp.int32, (cols, LANES), 0)
    lane = lax.broadcasted_iota(jnp.int32, (cols, LANES), 1)
    ritz = jnp.sum(jnp.where(lane == row, total, 0.0), axis=1, keepdims=True) + 1.0
    resid = jnp.sum(jnp.where(lane == row + cols, total, 0.0), axis=1, keepdims=True)
    factor = jnp.broadcast_to(jnp.sqrt(rows_total / ritz), (cols, LANES))
    norms = jnp.sqrt(resid / ritz)
    norm_ref[...] = jnp.sum(jnp.where(lane == row, norms, 0.0), axis=0, keepdims=True)
    me = lax.axis_index("grp")
    for s in range(groups):
        source = lax.rem(me + groups - s, groups)
        at = pl.ds(pl.multiple_of(source * LANES, LANES), LANES)
        for which in range(2):
            if s == 0:
                block = own_ref[which * cols : (which + 1) * cols]
                gain = factor
            else:
                ref = chunk_refs[s - 1]
                block = ref[pl.ds(which * cols * outer, cols * outer), :].reshape(cols, outer, LANES)
                exponent = ref[pl.ds(2 * cols * outer + which * cols, cols), :]
                gain = factor * power_of_two(exponent, -1)
            outs[which][:, :, at] = block * gain[:, None, :]


def shifted(value, s, groups):
    return lax.ppermute(value, "grp", [(i, (i + s) % groups) for i in range(groups)])


def everyone(value, axis):
    size = lax.axis_size(axis)
    copies = jnp.broadcast_to(value[None], (size, *value.shape))
    return lax.all_to_all(copies, axis, split_axis=0, concat_axis=0, tiled=True)


def body(krylov_basis, krylov_image, tridiag_vectors, ritz_values):
    groups = lax.axis_size("grp")
    krylov, outer, inner = krylov_basis.shape
    cols = tridiag_vectors.shape[1]
    rows_total = float(outer * inner * groups * lax.axis_size("row"))
    f32 = jnp.float32
    own_coefs = pl.pallas_call(
        pack_kernel, out_shape=jax.ShapeDtypeStruct((cols, SHIFT_AT + LANES), jnp.bfloat16), name="pack"
    )(tridiag_vectors.T, ritz_values[None, :])
    coefs = [own_coefs] + [shifted(own_coefs, groups - s, groups) for s in range(1, groups)]

    per_step = 16
    whole = lambda shape: pl.BlockSpec(shape, lambda j: (0,) * len(shape))
    field = pl.BlockSpec((krylov, per_step, inner), lambda j: (0, j, 0))
    chunk = (2 * cols * (outer + 1), LANES)
    shapes = [(2 * cols, outer, LANES)] + [chunk] * (groups - 1) + [(1, LANES)] * groups
    outs = pl.pallas_call(
        functools.partial(project_kernel, groups=groups, per_step=per_step),
        grid=(outer // per_step,),
        in_specs=[whole(own_coefs.shape)] * groups + [field] * 2,
        out_specs=[whole(shape) for shape in shapes],
        out_shape=[jax.ShapeDtypeStruct(shape, f32) for shape in shapes],
        scratch_shapes=[
            pltpu.VMEM((outer, 2 * groups * cols, LANES), f32),
            pltpu.VMEM((2 * groups * cols, 2 * LANES), f32),
            pltpu.VMEM((2 * groups * cols, 2 * LANES), f32),
        ],
        name="project",
    )(*coefs, krylov_basis, krylov_image)
    own, chunks, sums = outs[0], outs[1:groups], outs[groups:]
    total = sums[0] + sum(shifted(sums[s], s, groups) for s in range(1, groups))
    chunks = [shifted(c.astype(jnp.float16), s + 1, groups).astype(f32) for s, c in enumerate(chunks)]
    totals = everyone(total, "row").reshape(-1, LANES)
    ritz, resid, norms = pl.pallas_call(
        functools.partial(finish_kernel, groups=groups, rows_total=rows_total),
        out_shape=[jax.ShapeDtypeStruct((cols, outer, groups * inner), f32)] * 2
        + [jax.ShapeDtypeStruct((1, LANES), f32)],
        name="finish",
    )(own, *chunks, totals)
    return ritz, resid, norms[0, :cols]


def solution(mesh):
    placed = (P(None, "row", "grp"), P(None, "row", "grp"), P(None, "grp"), P("grp"))
    return jax.shard_map(
        body,
        mesh=mesh,
        in_specs=placed,
        out_specs=(P("grp", "row", None), P("grp", "row", None), P("grp")),
        check_vma=False,
    )
```

```python
import functools

import jax
import jax.numpy as jnp
from jax import lax
from jax.experimental import pallas as pl
from jax.experimental.pallas import tpu as pltpu
from jax.sharding import PartitionSpec as P


LANES = 128
SHIFT_AT = 384


def pack_kernel(coef_hbm, value_hbm, out_ref, coef_ref, value_ref, arrived):
    cols, krylov = coef_ref.shape
    copies = [
        pltpu.make_async_copy(coef_hbm, coef_ref, arrived.at[0]),
        pltpu.make_async_copy(value_hbm, value_ref, arrived.at[1]),
    ]
    for copy in copies:
        copy.start()
    out_ref[...] = jnp.zeros_like(out_ref)
    for copy in copies:
        copy.wait()
    out_ref[:, :krylov] = coef_ref[...]
    row = lax.broadcasted_iota(jnp.int32, (cols, cols), 0)
    lane = lax.broadcasted_iota(jnp.int32, (cols, cols), 1)
    values = jnp.broadcast_to(value_ref[...].astype(jnp.float32), (cols, cols))
    column = jnp.sum(jnp.where(row == lane, values, 0.0), axis=1, keepdims=True)
    out_ref[:, SHIFT_AT:] = jnp.broadcast_to(column, (cols, LANES)).astype(jnp.bfloat16)


def stage_kernel(basis_ref, image_ref, basis_out, image_out, landing, arrived, *, per_step):
    outer = basis_ref.shape[1]
    steps = outer // per_step
    copies = []
    for which, ref in enumerate((basis_ref, image_ref)):
        for j in range(steps):
            at = which * steps + j
            copy = pltpu.make_async_copy(
                ref.at[:, pl.ds(j * per_step, per_step), :], landing.at[at], arrived.at[at]
            )
            copy.start()
            copies.append(copy)
    for which, out in enumerate((basis_out, image_out)):
        for j in range(steps):
            at = which * steps + j
            copies[at].wait()
            out[pl.ds(j * per_step, per_step)] = jnp.swapaxes(landing[at], 0, 1)


def power_of_two(exponent, sign):
    out = jnp.ones(exponent.shape, jnp.float32)
    whole = exponent.astype(jnp.int32)
    for bit in range(7):
        out = out * jnp.where((whole & (1 << bit)) != 0, 2.0 ** (sign * (1 << bit)), 1.0)
    return out


def project_kernel(*refs, groups):
    coef_refs, (basis_ref, image_ref) = refs[:groups], refs[groups : groups + 2]
    own_ref = refs[groups + 2]
    chunk_refs = refs[groups + 3 : 2 * groups + 2]
    sum_ref, held = refs[2 * groups + 2 :]
    outer, krylov, _ = basis_ref.shape
    cols = coef_refs[0].shape[0]
    wanted = groups * cols
    coefs = jnp.concatenate([ref[:, :krylov].astype(jnp.float32) for ref in coef_refs])
    coefs = coefs.astype(jnp.bfloat16)
    shift = jnp.concatenate([ref[:, SHIFT_AT:].astype(jnp.float32) for ref in coef_refs])
    shift = jnp.concatenate([shift, shift], axis=1)
    zeros = jnp.zeros((wanted, 2 * LANES), jnp.float32)
    squares, peaks = [zeros, zeros], [zeros, zeros]
    for pair in range(0, outer, 2):
        fields = []
        for ref in (basis_ref, image_ref):
            both = jnp.concatenate([ref[pair], ref[pair + 1]], axis=1)
            fields.append(jnp.dot(coefs, both, preferred_element_type=jnp.float32))
        ritz, resid = fields[0], fields[1] - shift * fields[0]
        for which, value in enumerate((ritz, resid)):
            squares[which] += value * value
            peaks[which] = jnp.maximum(peaks[which], jnp.abs(value))
            for half in range(2):
                held[pair + half, pl.ds(which * wanted, wanted)] = value[:, half * LANES : (half + 1) * LANES]
    sums = [jnp.sum(x, axis=1, keepdims=True) for x in squares]
    row = lax.broadcasted_iota(jnp.int32, (wanted, LANES), 0)
    lane = lax.broadcasted_iota(jnp.int32, (wanted, LANES), 1)
    line = jnp.where(lane == row, sums[0], 0.0) + jnp.where(lane == row + wanted, sums[1], 0.0)
    sum_ref[...] = jnp.broadcast_to(jnp.sum(line, axis=0, keepdims=True), sum_ref.shape)
    for which in range(2):
        peak = jnp.max(peaks[which], axis=1, keepdims=True)
        exponent = jnp.clip(jnp.floor(14.0 - jnp.log(peak) * 1.4426950408889634), 0.0, 100.0)
        exponent = jnp.broadcast_to(exponent, (wanted, LANES))
        scale = power_of_two(exponent, 1)
        for s in range(groups):
            at = s * cols
            block = jnp.swapaxes(held[:, pl.ds(which * wanted + at, cols), :], 0, 1)
            if s == 0:
                own_ref[which * cols : (which + 1) * cols] = block
            else:
                block = block * scale[at : at + cols][:, None, :]
                ref = chunk_refs[s - 1]
                ref[pl.ds(which * cols * outer, cols * outer), :] = block.reshape(cols * outer, LANES)
                ref[pl.ds(2 * cols * outer + which * cols, cols), :] = exponent[at : at + cols]


def finish_kernel(*refs, groups, rows_total):
    own_ref, chunk_refs, line_refs = refs[0], refs[1:groups], refs[groups : 2 * groups]
    outs, norm_ref = refs[2 * groups : 2 * groups + 2], refs[2 * groups + 2]
    double, outer, _ = own_ref.shape
    cols = double // 2
    row = lax.broadcasted_iota(jnp.int32, (cols, LANES), 0)
    lane = lax.broadcasted_iota(jnp.int32, (cols, LANES), 1)
    ritz, resid = jnp.zeros((cols, LANES), jnp.float32), jnp.zeros((cols, LANES), jnp.float32)
    for s, ref in enumerate(line_refs):
        ritz += jnp.where(lane == row + s * cols, ref[...], 0.0)
        resid += jnp.where(lane == row + (s + groups) * cols, ref[...], 0.0)
    ritz = jnp.sum(ritz, axis=1, keepdims=True) + 1.0
    resid = jnp.sum(resid, axis=1, keepdims=True)
    factor = jnp.broadcast_to(jnp.sqrt(rows_total / ritz), (cols, LANES))
    norms = jnp.sqrt(resid / ritz)
    norm_ref[...] = jnp.sum(jnp.where(lane == row, norms, 0.0), axis=0, keepdims=True)[:, :cols]
    me = lax.axis_index("grp")
    for s in range(groups):
        source = lax.rem(me + groups - s, groups)
        at = pl.ds(pl.multiple_of(source * LANES, LANES), LANES)
        for which in range(2):
            if s == 0:
                block = own_ref[which * cols : (which + 1) * cols]
                gain = factor
            else:
                ref = chunk_refs[s - 1]
                block = ref[pl.ds(which * cols * outer, cols * outer), :].reshape(cols, outer, LANES)
                exponent = ref[pl.ds(2 * cols * outer + which * cols, cols), :]
                gain = factor * power_of_two(exponent, -1)
            outs[which][:, :, at] = block * gain[:, None, :]


def shifted(value, s, groups):
    return lax.ppermute(value, "grp", [(i, (i + s) % groups) for i in range(groups)])


def in_hbm(value):
    return pltpu.with_memory_space_constraint(value, pltpu.HBM)


def grant(mib):
    return pltpu.CompilerParams(vmem_limit_bytes=mib << 20)


def body(krylov_basis, krylov_image, tridiag_vectors, ritz_values):
    groups = lax.axis_size("grp")
    members = lax.axis_size("row")
    krylov, outer, inner = krylov_basis.shape
    cols = tridiag_vectors.shape[1]
    wanted = groups * cols
    rows_total = float(outer * inner * groups * members)
    f32 = jnp.float32
    own_coefs = pl.pallas_call(
        pack_kernel,
        out_shape=jax.ShapeDtypeStruct((cols, SHIFT_AT + LANES), jnp.bfloat16),
        in_specs=[pl.BlockSpec(memory_space=pltpu.HBM)] * 2,
        scratch_shapes=[
            pltpu.VMEM((cols, krylov), jnp.bfloat16),
            pltpu.VMEM((1, cols), jnp.bfloat16),
            pltpu.SemaphoreType.DMA((2,)),
        ],
        compiler_params=grant(1),
        name="pack",
    )(in_hbm(tridiag_vectors.T), in_hbm(ritz_values[None, :]))
    coefs = [own_coefs] + [shifted(own_coefs, groups - s, groups) for s in range(1, groups)]

    per_step = 16
    basis, image, _ = lax.optimization_barrier((krylov_basis, krylov_image, own_coefs))
    turned = jax.ShapeDtypeStruct((outer, krylov, inner), krylov_basis.dtype)
    basis, image = pl.pallas_call(
        functools.partial(stage_kernel, per_step=per_step),
        in_specs=[pl.BlockSpec(memory_space=pltpu.HBM)] * 2,
        out_shape=[turned] * 2,
        scratch_shapes=[
            pltpu.VMEM((2 * outer // per_step, krylov, per_step, inner), krylov_basis.dtype),
            pltpu.SemaphoreType.DMA((2 * outer // per_step,)),
        ],
        cost_estimate=pl.CostEstimate(flops=3 << 30, bytes_accessed=2 * krylov_basis.size * 2, transcendentals=0),
        compiler_params=grant(26),
        name="stage",
    )(in_hbm(basis), in_hbm(image))

    chunk = (2 * cols * (outer + 1), LANES)
    shapes = [(2 * cols, outer, LANES)] + [chunk] * (groups - 1) + [(members, LANES)]
    outs = pl.pallas_call(
        functools.partial(project_kernel, groups=groups),
        out_shape=[jax.ShapeDtypeStruct(shape, f32) for shape in shapes],
        scratch_shapes=[pltpu.VMEM((outer, 2 * wanted, LANES), f32)],
        compiler_params=grant(20),
        name="project",
    )(*coefs, basis, image)
    own, chunks, sums = outs[0], outs[1:groups], outs[groups]
    totals = lax.all_to_all(sums[:, None, :], "row", split_axis=0, concat_axis=0, tiled=True)
    sent = [shifted(c.astype(jnp.float16), s + 1, groups) for s, c in enumerate(chunks)]
    chunks = [c.astype(f32) for c in sent]
    total = totals.sum(axis=0)
    lines = [total] + [shifted(total, s, groups) for s in range(1, groups)]
    ritz, resid, norms = pl.pallas_call(
        functools.partial(finish_kernel, groups=groups, rows_total=rows_total),
        out_shape=[jax.ShapeDtypeStruct((cols, outer, groups * inner), f32)] * 2
        + [jax.ShapeDtypeStruct((1, cols), f32)],
        compiler_params=grant(12),
        name="finish",
    )(own, *chunks, *lines)
    return ritz, resid, norms.reshape(cols)


def solution(mesh):
    placed = (P(None, "row", "grp"), P(None, "row", "grp"), P(None, "grp"), P("grp"))
    return jax.shard_map(
        body,
        mesh=mesh,
        in_specs=placed,
        out_specs=(P("grp", "row", None), P("grp", "row", None), P("grp")),
        check_vma=False,
    )
```

```python
import functools

import jax
import jax.numpy as jnp
from jax import lax
from jax.experimental import pallas as pl
from jax.experimental.pallas import tpu as pltpu
from jax.sharding import PartitionSpec as P


LANES = 128
SHIFT_AT = 384
LEADER = 41


def pack_kernel(coef_hbm, value_hbm, out_ref, coef_ref, value_ref, arrived):
    cols, krylov = coef_ref.shape
    copies = [
        pltpu.make_async_copy(coef_hbm, coef_ref, arrived.at[0]),
        pltpu.make_async_copy(value_hbm, value_ref, arrived.at[1]),
    ]
    for copy in copies:
        copy.start()
    out_ref[...] = jnp.zeros_like(out_ref)
    for copy in copies:
        copy.wait()
    out_ref[:, :krylov] = coef_ref[...]
    row = lax.broadcasted_iota(jnp.int32, (cols, cols), 0)
    lane = lax.broadcasted_iota(jnp.int32, (cols, cols), 1)
    values = jnp.broadcast_to(value_ref[...].astype(jnp.float32), (cols, cols))
    column = jnp.sum(jnp.where(row == lane, values, 0.0), axis=1, keepdims=True)
    out_ref[:, SHIFT_AT:] = jnp.broadcast_to(column, (cols, LANES)).astype(jnp.bfloat16)


def stage_kernel(basis_ref, image_ref, basis_out, image_out):
    krylov, outer, _ = basis_ref.shape
    for ref, out in ((basis_ref, basis_out), (image_ref, image_out)):
        for j in range(0, outer, 8):
            for k in range(0, krylov, 16):
                some = min(16, krylov - k)
                block = ref[pl.ds(k, some), pl.ds(j, 8), :]
                out[pl.ds(j, 8), pl.ds(k, some), :] = jnp.swapaxes(block, 0, 1)


def power_of_two(exponent, sign):
    out = jnp.ones(exponent.shape, jnp.float32)
    whole = exponent.astype(jnp.int32)
    for bit in range(7):
        out = out * jnp.where((whole & (1 << bit)) != 0, 2.0 ** (sign * (1 << bit)), 1.0)
    return out


def project_kernel(*refs, groups):
    coef_refs, (basis_ref, image_ref) = refs[:groups], refs[groups : groups + 2]
    own_ref = refs[groups + 2]
    chunk_refs = refs[groups + 3 : 2 * groups + 2]
    sum_ref, held = refs[2 * groups + 2 :]
    outer, krylov, _ = basis_ref.shape
    cols = coef_refs[0].shape[0]
    wanted = groups * cols
    coefs = jnp.concatenate([ref[:, :krylov].astype(jnp.float32) for ref in coef_refs])
    coefs = coefs.astype(jnp.bfloat16)
    shift = jnp.concatenate([ref[:, SHIFT_AT:].astype(jnp.float32) for ref in coef_refs])
    shift = jnp.concatenate([shift, shift], axis=1)
    zeros = jnp.zeros((wanted, 2 * LANES), jnp.float32)
    squares, peaks = [zeros, zeros], [zeros, zeros]
    for pair in range(0, outer, 2):
        fields = []
        for ref in (basis_ref, image_ref):
            both = jnp.concatenate([ref[pair], ref[pair + 1]], axis=1)
            fields.append(jnp.dot(coefs, both, preferred_element_type=jnp.float32))
        ritz, resid = fields[0], fields[1] - shift * fields[0]
        for which, value in enumerate((ritz, resid)):
            squares[which] += value * value
            peaks[which] = jnp.maximum(peaks[which], jnp.abs(value))
            for half in range(2):
                held[pair + half, pl.ds(which * wanted, wanted)] = value[:, half * LANES : (half + 1) * LANES]
    sums = [jnp.sum(x, axis=1, keepdims=True) for x in squares]
    row = lax.broadcasted_iota(jnp.int32, (wanted, LANES), 0)
    lane = lax.broadcasted_iota(jnp.int32, (wanted, LANES), 1)
    line = jnp.where(lane == row, sums[0], 0.0) + jnp.where(lane == row + wanted, sums[1], 0.0)
    sum_ref[...] = jnp.broadcast_to(jnp.sum(line, axis=0, keepdims=True), sum_ref.shape)
    for which in range(2):
        peak = jnp.max(peaks[which], axis=1, keepdims=True)
        exponent = jnp.clip(jnp.floor(14.0 - jnp.log(peak) * 1.4426950408889634), 0.0, 100.0)
        exponent = jnp.broadcast_to(exponent, (wanted, LANES))
        scale = power_of_two(exponent, 1)
        for s in range(groups):
            at = s * cols
            block = jnp.swapaxes(held[:, pl.ds(which * wanted + at, cols), :], 0, 1)
            if s == 0:
                own_ref[which * cols : (which + 1) * cols] = block
            else:
                block = block * scale[at : at + cols][:, None, :]
                ref = chunk_refs[s - 1]
                ref[pl.ds(which * cols * outer, cols * outer), :] = block.reshape(cols * outer, LANES)
                ref[pl.ds(2 * cols * outer + which * cols, cols), :] = exponent[at : at + cols]


def finish_kernel(*refs, groups, rows_total):
    own_ref, chunk_refs, line_refs = refs[0], refs[1:groups], refs[groups:-3]
    outs, norm_ref = refs[-3:-1], refs[-1]
    double, outer, _ = own_ref.shape
    cols = double // 2
    row = lax.broadcasted_iota(jnp.int32, (cols, LANES), 0)
    lane = lax.broadcasted_iota(jnp.int32, (cols, LANES), 1)
    ritz, resid = jnp.zeros((cols, LANES), jnp.float32), jnp.zeros((cols, LANES), jnp.float32)
    for s, ref in enumerate(line_refs):
        ritz += jnp.where(lane == row + s * cols, ref[...], 0.0)
        resid += jnp.where(lane == row + (s + groups) * cols, ref[...], 0.0)
    ritz = jnp.sum(ritz, axis=1, keepdims=True) + 1.0
    resid = jnp.sum(resid, axis=1, keepdims=True)
    factor = jnp.broadcast_to(jnp.sqrt(rows_total / ritz), (cols, LANES))
    norms = jnp.sqrt(resid / ritz)
    norm_ref[...] = jnp.sum(jnp.where(lane == row, norms, 0.0), axis=0, keepdims=True)[:, :cols]
    me = lax.axis_index("grp")
    for s in range(groups):
        source = lax.rem(me + groups - s, groups)
        at = pl.ds(pl.multiple_of(source * LANES, LANES), LANES)
        for which in range(2):
            if s == 0:
                block = own_ref[which * cols : (which + 1) * cols]
                gain = factor
            else:
                ref = chunk_refs[s - 1]
                block = ref[pl.ds(which * cols * outer, cols * outer), :].reshape(cols, outer, LANES)
                exponent = ref[pl.ds(2 * cols * outer + which * cols, cols), :]
                gain = factor * power_of_two(exponent, -1)
            outs[which][:, :, at] = block * gain[:, None, :]


def shifted(value, s, groups):
    return lax.ppermute(value, "grp", [(i, (i + s) % groups) for i in range(groups)])


def in_hbm(value):
    return pltpu.with_memory_space_constraint(value, pltpu.HBM)


def grant(mib):
    return pltpu.CompilerParams(vmem_limit_bytes=mib << 20)


def body(krylov_basis, krylov_image, tridiag_vectors, ritz_values):
    groups = lax.axis_size("grp")
    members = lax.axis_size("row")
    krylov, outer, inner = krylov_basis.shape
    cols = tridiag_vectors.shape[1]
    wanted = groups * cols
    rows_total = float(outer * inner * groups * members)
    f32 = jnp.float32
    own_coefs = pl.pallas_call(
        pack_kernel,
        out_shape=jax.ShapeDtypeStruct((cols, SHIFT_AT + LANES), jnp.bfloat16),
        in_specs=[pl.BlockSpec(memory_space=pltpu.HBM)] * 2,
        scratch_shapes=[
            pltpu.VMEM((cols, krylov), jnp.bfloat16),
            pltpu.VMEM((1, cols), jnp.bfloat16),
            pltpu.SemaphoreType.DMA((2,)),
        ],
        cost_estimate=pl.CostEstimate(flops=6 << 30, bytes_accessed=16 << 20, transcendentals=0),
        compiler_params=grant(1),
        name="pack",
    )(in_hbm(tridiag_vectors.T), in_hbm(ritz_values[None, :]))
    coefs = [own_coefs] + [shifted(own_coefs, groups - s, groups) for s in range(1, groups)]

    basis, image = krylov_basis, krylov_image
    turned = jax.ShapeDtypeStruct((outer, krylov, inner), krylov_basis.dtype)
    basis, image = pl.pallas_call(
        stage_kernel,
        out_shape=[turned] * 2,
        cost_estimate=pl.CostEstimate(flops=3 << 30, bytes_accessed=2 * krylov_basis.size * 2, transcendentals=0),
        compiler_params=grant(4),
        name="stage",
    )(basis, image)

    chunk = (2 * cols * (outer + 1), LANES)
    shapes = [(2 * cols, outer, LANES)] + [chunk] * (groups - 1) + [(members, LANES)]
    outs = pl.pallas_call(
        functools.partial(project_kernel, groups=groups),
        out_shape=[jax.ShapeDtypeStruct(shape, f32) for shape in shapes],
        scratch_shapes=[pltpu.VMEM((outer, 2 * wanted, LANES), f32)],
        compiler_params=grant(20),
        name="project",
    )(*coefs, basis, image)
    own, chunks, sums = outs[0], outs[1:groups], outs[groups]
    sent = [shifted(c.astype(jnp.float16), s + 1, groups) for s, c in enumerate(chunks)]
    chunks = [c.astype(f32) for c in sent]
    line = sums[:1]
    moved = [line] + [shifted(line, s, groups) for s in range(1, groups)]
    wide = lax.broadcasted_iota(jnp.int32, (1, LANES), 1)
    total = jnp.zeros((1, LANES), f32)
    for s, m in enumerate(moved):
        here = (wide // cols) % groups == s
        total = total + jnp.roll(jnp.where(here, m, 0.0), -s * cols, axis=1)
    totals = lax.all_to_all(jnp.broadcast_to(total[None], (members, 1, LANES)), "row", split_axis=0, concat_axis=0, tiled=True, axis_index_groups=[[(r + LEADER) % members for r in range(members)]])
    lines = [totals.sum(axis=0)]
    ritz, resid, norms = pl.pallas_call(
        functools.partial(finish_kernel, groups=groups, rows_total=rows_total),
        out_shape=[jax.ShapeDtypeStruct((cols, outer, groups * inner), f32)] * 2
        + [jax.ShapeDtypeStruct((1, cols), f32)],
        compiler_params=grant(12),
        name="finish",
    )(own, *chunks, *lines)
    return ritz, resid, norms.reshape(cols)


def solution(mesh):
    placed = (P(None, "row", "grp"), P(None, "row", "grp"), P(None, "grp"), P("grp"))
    return jax.shard_map(
        body,
        mesh=mesh,
        in_specs=placed,
        out_specs=(P("grp", "row", None), P("grp", "row", None), P("grp")),
        check_vma=False,
    )
```

```python
import functools

import jax
import jax.numpy as jnp
from jax import lax
from jax.experimental import pallas as pl
from jax.experimental.pallas import tpu as pltpu
from jax.sharding import PartitionSpec as P


LANES = 128
SHIFT_AT = 384
LEADER = 41


def pack_kernel(coef_hbm, value_hbm, out_ref, coef_ref, value_ref, arrived):
    cols, krylov = coef_ref.shape
    copies = [
        pltpu.make_async_copy(coef_hbm, coef_ref, arrived.at[0]),
        pltpu.make_async_copy(value_hbm, value_ref, arrived.at[1]),
    ]
    for copy in copies:
        copy.start()
    out_ref[...] = jnp.zeros_like(out_ref)
    for copy in copies:
        copy.wait()
    out_ref[:, :krylov] = coef_ref[...]
    row = lax.broadcasted_iota(jnp.int32, (cols, cols), 0)
    lane = lax.broadcasted_iota(jnp.int32, (cols, cols), 1)
    values = jnp.broadcast_to(value_ref[...].astype(jnp.float32), (cols, cols))
    column = jnp.sum(jnp.where(row == lane, values, 0.0), axis=1, keepdims=True)
    out_ref[:, SHIFT_AT:] = jnp.broadcast_to(column, (cols, LANES)).astype(jnp.bfloat16)


def stage_kernel(basis_ref, image_ref, basis_out, image_out):
    krylov, outer, _ = basis_ref.shape
    for ref, out in ((basis_ref, basis_out), (image_ref, image_out)):
        for j in range(0, outer, 8):
            for k in range(0, krylov, 16):
                some = min(16, krylov - k)
                block = ref[pl.ds(k, some), pl.ds(j, 8), :]
                out[pl.ds(j, 8), pl.ds(k, some), :] = jnp.swapaxes(block, 0, 1)


def power_of_two(exponent, sign):
    out = jnp.ones(exponent.shape, jnp.float32)
    whole = exponent.astype(jnp.int32)
    for bit in range(7):
        out = out * jnp.where((whole & (1 << bit)) != 0, 2.0 ** (sign * (1 << bit)), 1.0)
    return out


def project_kernel(*refs, groups):
    coef_refs, (basis_ref, image_ref) = refs[:groups], refs[groups : groups + 2]
    own_ref = refs[groups + 2]
    chunk_refs = refs[groups + 3 : 2 * groups + 2]
    sum_ref, held = refs[2 * groups + 2 :]
    outer, krylov, _ = basis_ref.shape
    cols = coef_refs[0].shape[0]
    wanted = groups * cols
    coefs = jnp.concatenate([ref[:, :krylov].astype(jnp.float32) for ref in coef_refs])
    coefs = coefs.astype(jnp.bfloat16)
    shift = jnp.concatenate([ref[:, SHIFT_AT:].astype(jnp.float32) for ref in coef_refs])
    shift = jnp.concatenate([shift, shift], axis=1)
    zeros = jnp.zeros((wanted, LANES), jnp.float32)
    squares, peaks = [zeros, zeros], [zeros, zeros]
    for pair in range(0, outer, 2):
        fields = []
        for ref in (basis_ref, image_ref):
            both = jnp.concatenate([ref[pair], ref[pair + 1]], axis=1)
            fields.append(jnp.dot(coefs, both, preferred_element_type=jnp.float32))
        ritz, resid = fields[0], fields[1] - shift * fields[0]
        for which, value in enumerate((ritz, resid)):
            for half in range(2):
                part = value[:, half * LANES : (half + 1) * LANES]
                squares[which] += part * part
                peaks[which] = jnp.maximum(peaks[which], jnp.abs(part))
                held[pair + half, pl.ds(which * wanted, wanted)] = part
    sums = [jnp.sum(x, axis=1, keepdims=True) for x in squares]
    row = lax.broadcasted_iota(jnp.int32, (wanted, LANES), 0)
    lane = lax.broadcasted_iota(jnp.int32, (wanted, LANES), 1)
    line = jnp.where(lane == row, sums[0], 0.0) + jnp.where(lane == row + wanted, sums[1], 0.0)
    sum_ref[...] = jnp.broadcast_to(jnp.sum(line, axis=0, keepdims=True), sum_ref.shape)
    for which in range(2):
        peak = jnp.max(peaks[which], axis=1, keepdims=True)
        exponent = jnp.clip(jnp.floor(14.0 - jnp.log(peak) * 1.4426950408889634), 0.0, 100.0)
        exponent = jnp.broadcast_to(exponent, (wanted, LANES))
        scale = power_of_two(exponent, 1)
        for s in range(groups):
            at = s * cols
            block = jnp.swapaxes(held[:, pl.ds(which * wanted + at, cols), :], 0, 1)
            if s == 0:
                own_ref[which * cols : (which + 1) * cols] = block
            else:
                block = block * scale[at : at + cols][:, None, :]
                ref = chunk_refs[s - 1]
                ref[pl.ds(which * cols * outer, cols * outer), :] = block.reshape(cols * outer, LANES)
                ref[pl.ds(2 * cols * outer + which * cols, cols), :] = exponent[at : at + cols]


def finish_kernel(*refs, groups, rows_total):
    own_ref, chunk_refs, line_refs = refs[0], refs[1:groups], refs[groups:-3]
    outs, norm_ref = refs[-3:-1], refs[-1]
    double, outer, _ = own_ref.shape
    cols = double // 2
    row = lax.broadcasted_iota(jnp.int32, (cols, LANES), 0)
    lane = lax.broadcasted_iota(jnp.int32, (cols, LANES), 1)
    ritz, resid = jnp.zeros((cols, LANES), jnp.float32), jnp.zeros((cols, LANES), jnp.float32)
    for s, ref in enumerate(line_refs):
        ritz += jnp.where(lane == row + s * cols, ref[...], 0.0)
        resid += jnp.where(lane == row + (s + groups) * cols, ref[...], 0.0)
    ritz = jnp.sum(ritz, axis=1, keepdims=True) + 1.0
    resid = jnp.sum(resid, axis=1, keepdims=True)
    factor = jnp.broadcast_to(jnp.sqrt(rows_total / ritz), (cols, LANES))
    norms = jnp.sqrt(resid / ritz)
    norm_ref[...] = jnp.sum(jnp.where(lane == row, norms, 0.0), axis=0, keepdims=True)[:, :cols]
    me = lax.axis_index("grp")
    for s in range(groups):
        source = me ^ s
        at = pl.ds(pl.multiple_of(source * LANES, LANES), LANES)
        for which in range(2):
            if s == 0:
                block = own_ref[which * cols : (which + 1) * cols]
                gain = factor
            else:
                ref = chunk_refs[s - 1]
                block = ref[pl.ds(which * cols * outer, cols * outer), :].reshape(cols, outer, LANES)
                exponent = ref[pl.ds(2 * cols * outer + which * cols, cols), :]
                gain = factor * power_of_two(exponent, -1)
            outs[which][:, :, at] = block * gain[:, None, :]


def total_kernel(*refs, cols):
    line_refs, out_ref = refs[:-1], refs[-1]
    groups = len(line_refs)
    total = jnp.zeros((1, LANES), jnp.float32)
    lane = lax.broadcasted_iota(jnp.int32, (1, LANES), 1)
    for s, ref in enumerate(line_refs):
        mine = jnp.where((lane // cols) % groups == s, ref[...], 0.0)
        total = total + (mine if s == 0 else pltpu.roll(mine, LANES - s * cols, 1))
    out_ref[...] = jnp.broadcast_to(total, out_ref.shape)


def shifted(value, s, groups):
    return lax.ppermute(value, "grp", [(i, i ^ s) for i in range(groups)])


def in_hbm(value):
    return pltpu.with_memory_space_constraint(value, pltpu.HBM)


def grant(mib):
    return pltpu.CompilerParams(vmem_limit_bytes=mib << 20)


def body(krylov_basis, krylov_image, tridiag_vectors, ritz_values):
    groups = lax.axis_size("grp")
    members = lax.axis_size("row")
    krylov, outer, inner = krylov_basis.shape
    cols = tridiag_vectors.shape[1]
    wanted = groups * cols
    rows_total = float(outer * inner * groups * members)
    f32 = jnp.float32
    own_coefs = pl.pallas_call(
        pack_kernel,
        out_shape=jax.ShapeDtypeStruct((cols, SHIFT_AT + LANES), jnp.bfloat16),
        in_specs=[pl.BlockSpec(memory_space=pltpu.HBM)] * 2,
        scratch_shapes=[
            pltpu.VMEM((cols, krylov), jnp.bfloat16),
            pltpu.VMEM((1, cols), jnp.bfloat16),
            pltpu.SemaphoreType.DMA((2,)),
        ],
        cost_estimate=pl.CostEstimate(flops=6 << 30, bytes_accessed=16 << 20, transcendentals=0),
        compiler_params=grant(1),
        name="pack",
    )(in_hbm(tridiag_vectors.T), in_hbm(ritz_values[None, :]))
    coefs = [own_coefs] + [shifted(own_coefs, s, groups) for s in range(1, groups)]

    basis, image = krylov_basis, krylov_image
    turned = jax.ShapeDtypeStruct((outer, krylov, inner), krylov_basis.dtype)
    basis, image = pl.pallas_call(
        stage_kernel,
        out_shape=[turned] * 2,
        cost_estimate=pl.CostEstimate(flops=3 << 30, bytes_accessed=2 * krylov_basis.size * 2, transcendentals=0),
        compiler_params=grant(4),
        name="stage",
    )(basis, image)

    chunk = (2 * cols * (outer + 1), LANES)
    shapes = [(2 * cols, outer, LANES)] + [chunk] * (groups - 1) + [(1, LANES)]
    outs = pl.pallas_call(
        functools.partial(project_kernel, groups=groups),
        out_shape=[jax.ShapeDtypeStruct(shape, f32) for shape in shapes],
        scratch_shapes=[pltpu.VMEM((outer, 2 * wanted, LANES), f32)],
        compiler_params=grant(20),
        name="project",
    )(*coefs, basis, image)
    own, chunks, sums = outs[0], outs[1:groups], outs[groups]
    sent = []
    for s, c in enumerate(chunks):
        sent.append(shifted(c.astype(jnp.float16), s + 1, groups))
    chunks = [c.astype(f32) for c in sent]
    line = sums
    moved = [line] + [shifted(line, s, groups) for s in range(1, groups)]
    spread = pl.pallas_call(
        functools.partial(total_kernel, cols=cols),
        out_shape=jax.ShapeDtypeStruct((members, LANES), f32),
        compiler_params=grant(1),
        name="total",
    )(*moved)
    totals = lax.all_to_all(spread[:, None, :], "row", split_axis=0, concat_axis=0, tiled=True, axis_index_groups=[[(r + LEADER) % members for r in range(members)]])
    lines = [totals.sum(axis=0)]
    ritz, resid, norms = pl.pallas_call(
        functools.partial(finish_kernel, groups=groups, rows_total=rows_total),
        out_shape=[jax.ShapeDtypeStruct((cols, outer, groups * inner), f32)] * 2
        + [jax.ShapeDtypeStruct((1, cols), f32)],
        compiler_params=grant(12),
        name="finish",
    )(own, *chunks, *lines)
    return ritz, resid, norms.reshape(cols)


def solution(mesh):
    placed = (P(None, "row", "grp"), P(None, "row", "grp"), P(None, "grp"), P("grp"))
    return jax.shard_map(
        body,
        mesh=mesh,
        in_specs=placed,
        out_specs=(P("grp", "row", None), P("grp", "row", None), P("grp")),
        check_vma=False,
    )
```

```python
import functools

import jax
import jax.numpy as jnp
from jax import lax
from jax.experimental import pallas as pl
from jax.experimental.pallas import tpu as pltpu
from jax.sharding import PartitionSpec as P


LANES = 128
SHIFT_AT = 384
LEADER = 41


def pack_kernel(coef_hbm, value_hbm, out_ref, coef_ref, value_ref, arrived):
    cols, krylov = coef_ref.shape
    copies = [
        pltpu.make_async_copy(coef_hbm, coef_ref, arrived.at[0]),
        pltpu.make_async_copy(value_hbm, value_ref, arrived.at[1]),
    ]
    for copy in copies:
        copy.start()
    out_ref[...] = jnp.zeros_like(out_ref)
    for copy in copies:
        copy.wait()
    out_ref[:, :krylov] = coef_ref[...]
    row = lax.broadcasted_iota(jnp.int32, (cols, cols), 0)
    lane = lax.broadcasted_iota(jnp.int32, (cols, cols), 1)
    values = jnp.broadcast_to(value_ref[...].astype(jnp.float32), (cols, cols))
    column = jnp.sum(jnp.where(row == lane, values, 0.0), axis=1, keepdims=True)
    out_ref[:, SHIFT_AT:] = jnp.broadcast_to(column, (cols, LANES)).astype(jnp.bfloat16)


def stage_kernel(basis_ref, image_ref, basis_out, image_out):
    krylov, outer, _ = basis_ref.shape
    for ref, out in ((basis_ref, basis_out), (image_ref, image_out)):
        for j in range(0, outer, 8):
            for k in range(0, krylov, 16):
                some = min(16, krylov - k)
                block = ref[pl.ds(k, some), pl.ds(j, 8), :]
                out[pl.ds(j, 8), pl.ds(k, some), :] = jnp.swapaxes(block, 0, 1)


def power_of_two(exponent, sign):
    out = jnp.ones(exponent.shape, jnp.float32)
    whole = exponent.astype(jnp.int32)
    for bit in range(7):
        out = out * jnp.where((whole & (1 << bit)) != 0, 2.0 ** (sign * (1 << bit)), 1.0)
    return out


def project_kernel(*refs, groups):
    coef_refs, (basis_ref, image_ref) = refs[:groups], refs[groups : groups + 2]
    own_ref = refs[groups + 2]
    chunk_refs = refs[groups + 3 : 2 * groups + 2]
    sum_ref, held = refs[2 * groups + 2 :]
    outer, krylov, _ = basis_ref.shape
    cols = coef_refs[0].shape[0]
    wanted = groups * cols
    coefs = jnp.concatenate([ref[:, :krylov].astype(jnp.float32) for ref in coef_refs])
    coefs = coefs.astype(jnp.bfloat16)
    shift = jnp.concatenate([ref[:, SHIFT_AT:].astype(jnp.float32) for ref in coef_refs])
    shift = jnp.concatenate([shift, shift], axis=1)
    zeros = jnp.zeros((wanted, LANES), jnp.float32)
    squares, peaks = [zeros, zeros], [zeros, zeros]
    for pair in range(0, outer, 2):
        fields = []
        for ref in (basis_ref, image_ref):
            both = jnp.concatenate([ref[pair], ref[pair + 1]], axis=1)
            fields.append(jnp.dot(coefs, both, preferred_element_type=jnp.float32))
        ritz, resid = fields[0], fields[1] - shift * fields[0]
        for which, value in enumerate((ritz, resid)):
            for half in range(2):
                part = value[:, half * LANES : (half + 1) * LANES]
                squares[which] += part * part
                peaks[which] = jnp.maximum(peaks[which], jnp.abs(part))
                held[pair + half, pl.ds(which * wanted, wanted)] = part
    sums = [jnp.sum(x, axis=1, keepdims=True) for x in squares]
    row = lax.broadcasted_iota(jnp.int32, (wanted, LANES), 0)
    lane = lax.broadcasted_iota(jnp.int32, (wanted, LANES), 1)
    line = jnp.where(lane == row, sums[0], 0.0) + jnp.where(lane == row + wanted, sums[1], 0.0)
    sum_ref[...] = jnp.broadcast_to(jnp.sum(line, axis=0, keepdims=True), sum_ref.shape)
    for which in range(2):
        peak = jnp.max(peaks[which], axis=1, keepdims=True)
        exponent = jnp.clip(jnp.floor(14.0 - jnp.log(peak) * 1.4426950408889634), 0.0, 100.0)
        exponent = jnp.broadcast_to(exponent, (wanted, LANES))
        scale = power_of_two(exponent, 1)
        for s in range(groups):
            at = s * cols
            block = jnp.swapaxes(held[:, pl.ds(which * wanted + at, cols), :], 0, 1)
            if s == 0:
                own_ref[which * cols : (which + 1) * cols] = block
            else:
                block = block * scale[at : at + cols][:, None, :]
                ref = chunk_refs[s - 1]
                ref[pl.ds(which * cols * outer, cols * outer), :] = block.reshape(cols * outer, LANES)
                ref[pl.ds(2 * cols * outer + which * cols, cols), :] = exponent[at : at + cols]


def assemble_kernel(*refs, groups):
    own_ref, chunk_refs, outs = refs[0], refs[1:groups], refs[groups:]
    double, outer, _ = own_ref.shape
    cols = double // 2
    me = lax.axis_index("grp")
    for s in range(groups):
        source = me ^ s
        at = pl.ds(pl.multiple_of(source * LANES, LANES), LANES)
        for which in range(2):
            if s == 0:
                outs[which][:, :, at] = own_ref[which * cols : (which + 1) * cols]
            else:
                ref = chunk_refs[s - 1]
                block = ref[pl.ds(which * cols * outer, cols * outer), :].reshape(cols, outer, LANES)
                exponent = ref[pl.ds(2 * cols * outer + which * cols, cols), :]
                outs[which][:, :, at] = block * power_of_two(exponent, -1)[:, None, :]


def finish_kernel(ritz_ref, resid_ref, line_ref, ritz_out, resid_out, norm_out, held, norm_ref, sent, *, groups, rows_total, per_copy):
    cols, _, inner = ritz_ref.shape
    row = lax.broadcasted_iota(jnp.int32, (cols, LANES), 0)
    lane = lax.broadcasted_iota(jnp.int32, (cols, LANES), 1)
    line = line_ref[...]
    ritz = jnp.sum(jnp.where(lane == row, line, 0.0), axis=1, keepdims=True) + 1.0
    resid = jnp.sum(jnp.where(lane == row + groups * cols, line, 0.0), axis=1, keepdims=True)
    factor = jnp.broadcast_to(jnp.sqrt(rows_total / ritz), (cols, LANES))
    norms = jnp.sqrt(resid / ritz)
    norm_ref[...] = jnp.sum(jnp.where(lane == row, norms, 0.0), axis=0, keepdims=True)[:, :cols]
    copies = [pltpu.make_async_copy(norm_ref, norm_out, sent.at[0])]
    copies[0].start()
    for which, (ref, out) in enumerate(((ritz_ref, ritz_out), (resid_ref, resid_out))):
        for i in range(0, cols, per_copy):
            rows = pl.ds(i, per_copy)
            for at in range(0, inner, LANES):
                lanes = pl.ds(at, LANES)
                held[which, rows, :, lanes] = ref[rows, :, lanes] * factor[i : i + per_copy][:, None, :]
            copy = pltpu.make_async_copy(held.at[which, rows], out.at[rows], sent.at[len(copies)])
            copy.start()
            copies.append(copy)
    for copy in copies:
        copy.wait()


def total_kernel(*refs, cols):
    line_refs, out_ref = refs[:-1], refs[-1]
    groups = len(line_refs)
    total = jnp.zeros((1, LANES), jnp.float32)
    lane = lax.broadcasted_iota(jnp.int32, (1, LANES), 1)
    for s, ref in enumerate(line_refs):
        mine = jnp.where((lane // cols) % groups == s, ref[...], 0.0)
        total = total + (mine if s == 0 else pltpu.roll(mine, LANES - s * cols, 1))
    out_ref[...] = jnp.broadcast_to(total, out_ref.shape)


def shifted(value, s, groups):
    return lax.ppermute(value, "grp", [(i, i ^ s) for i in range(groups)])


def in_hbm(value):
    return pltpu.with_memory_space_constraint(value, pltpu.HBM)


def grant(mib):
    return pltpu.CompilerParams(vmem_limit_bytes=mib << 20)


def body(krylov_basis, krylov_image, tridiag_vectors, ritz_values):
    groups = lax.axis_size("grp")
    members = lax.axis_size("row")
    krylov, outer, inner = krylov_basis.shape
    cols = tridiag_vectors.shape[1]
    wanted = groups * cols
    rows_total = float(outer * inner * groups * members)
    f32 = jnp.float32
    own_coefs = pl.pallas_call(
        pack_kernel,
        out_shape=jax.ShapeDtypeStruct((cols, SHIFT_AT + LANES), jnp.bfloat16),
        in_specs=[pl.BlockSpec(memory_space=pltpu.HBM)] * 2,
        scratch_shapes=[
            pltpu.VMEM((cols, krylov), jnp.bfloat16),
            pltpu.VMEM((1, cols), jnp.bfloat16),
            pltpu.SemaphoreType.DMA((2,)),
        ],
        cost_estimate=pl.CostEstimate(flops=6 << 30, bytes_accessed=16 << 20, transcendentals=0),
        compiler_params=grant(1),
        name="pack",
    )(in_hbm(tridiag_vectors.T), in_hbm(ritz_values[None, :]))
    coefs = [own_coefs] + [shifted(own_coefs, s, groups) for s in range(1, groups)]

    basis, image = krylov_basis, krylov_image
    turned = jax.ShapeDtypeStruct((outer, krylov, inner), krylov_basis.dtype)
    basis, image = pl.pallas_call(
        stage_kernel,
        out_shape=[turned] * 2,
        cost_estimate=pl.CostEstimate(flops=3 << 30, bytes_accessed=2 * krylov_basis.size * 2, transcendentals=0),
        compiler_params=grant(4),
        name="stage",
    )(basis, image)

    chunk = (2 * cols * (outer + 1), LANES)
    shapes = [(2 * cols, outer, LANES)] + [chunk] * (groups - 1) + [(1, LANES)]
    outs = pl.pallas_call(
        functools.partial(project_kernel, groups=groups),
        out_shape=[jax.ShapeDtypeStruct(shape, f32) for shape in shapes],
        scratch_shapes=[pltpu.VMEM((outer, 2 * wanted, LANES), f32)],
        compiler_params=grant(20),
        name="project",
    )(*coefs, basis, image)
    own, chunks, sums = outs[0], outs[1:groups], outs[groups]
    sent = []
    for s, c in enumerate(chunks):
        sent.append(shifted(c.astype(jnp.float16), s + 1, groups))
    chunks = [c.astype(f32) for c in sent]
    full = jax.ShapeDtypeStruct((cols, outer, groups * inner), f32)
    ritz, resid = pl.pallas_call(
        functools.partial(assemble_kernel, groups=groups),
        out_shape=[full] * 2,
        compiler_params=grant(4),
        name="assemble",
    )(own, *chunks)
    line = sums
    moved = [line] + [shifted(line, s, groups) for s in range(1, groups)]
    spread = pl.pallas_call(
        functools.partial(total_kernel, cols=cols),
        out_shape=jax.ShapeDtypeStruct((members, LANES), f32),
        compiler_params=grant(1),
        name="total",
    )(*moved)
    totals = lax.all_to_all(spread[:, None, :], "row", split_axis=0, concat_axis=0, tiled=True, axis_index_groups=[[(r + LEADER) % members for r in range(members)]])
    lines = [totals.sum(axis=0)]
    ritz, resid, norms = pl.pallas_call(
        functools.partial(finish_kernel, groups=groups, rows_total=rows_total, per_copy=2),
        out_specs=[pl.BlockSpec(memory_space=pltpu.HBM)] * 3,
        out_shape=[full] * 2 + [jax.ShapeDtypeStruct((1, cols), f32)],
        scratch_shapes=[
            pltpu.VMEM((2, cols, outer, groups * inner), f32),
            pltpu.VMEM((1, cols), f32),
            pltpu.SemaphoreType.DMA((1 + 2 * cols // 2,)),
        ],
        compiler_params=grant(6),
        name="finish",
    )(ritz, resid, *lines)
    return ritz, resid, norms.reshape(cols)


def solution(mesh):
    placed = (P(None, "row", "grp"), P(None, "row", "grp"), P(None, "grp"), P("grp"))
    return jax.shard_map(
        body,
        mesh=mesh,
        in_specs=placed,
        out_specs=(P("grp", "row", None), P("grp", "row", None), P("grp")),
        check_vma=False,
    )
```
